32 devices in a mesh: tm: 16 (over z, y, x), rows: 2 (over core).
Axes of the slice: x: 2, y: 2, z: 4, core: 2. Of those that a mesh axis runs over, the one named last changes fastest.
Arguments:
- resid: float32 [2, 16, 16, 512], P(None, 'tm', 'rows'), may hold values from -3 to 3
- basis: float32 [4, 2, 16, 16, 512], P(None, None, 'tm', 'rows'), may hold values from -0.01171875 to 0.01171875
Outputs:
- precond: float32 [2, 16, 16, 512], P(None, 'tm', 'rows')
- image: float32 [2, 16, 16, 512], P(None, 'tm', 'rows')
- gram: float32 [5], replicated
The draws below stay inside these ranges and needn't reach their ends.
All inputs are finite; a program needn't handle non-finite values.
Results may differ from the reference program's by a relative error of at most 0.0005.
Values sent between devices are 32-bit elements; how exact they have to be, the bound alone decides.
A program may use at most 64 MiB of HBM per device.

```python
import jax
import jax.numpy as jnp

NY = 512
SWEEPS = 4
KRYLOV = 4
STEPS = 16
NX = 16


def block_scale(key, extent, pieces, low, top_value):
    loudness, own = 1.0, jax.random.fold_in(key, 6)
    for axis_at, shards_of in pieces:
        heights = jnp.exp(jax.random.uniform(jax.random.fold_in(own, axis_at), (shards_of,), jnp.float32, low / len(pieces), top_value / len(pieces)))
        loudness = loudness * jnp.repeat(heights, extent[axis_at] // shards_of).reshape([-1 if axis == axis_at else 1 for axis in range(len(extent))])
    return loudness


def centred(own_key, shape, spread, bound, shards=(), held_as=jnp.bfloat16):
    array = spread * jax.random.normal(own_key, shape, jnp.float32)
    if shards:
        array = array * block_scale(own_key, shape, shards, -0.22, 0.18)
    return jnp.clip(array, -bound, bound).astype(held_as)


def setup_inputs(seed: int = 0) -> dict:
    key_of = jax.random.split(jax.random.key(seed), 3)
    resid = centred(key_of[0], (2, STEPS, NX, NY), 0.5, 3.0, ((1, 16), (2, 2)), jnp.float32)
    basis = centred(key_of[1], (KRYLOV, 2, STEPS, NX, NY), (1.0 / (2 * STEPS * NX * NY) ** 0.5), 0.01171875, ((2, 16), (3, 2)), jnp.float32)
    return {"resid": resid, "basis": basis}


ALPHA = 0.01


def neighbours(field):
    padded = jnp.pad(field, ((0, 0), (1, 1), (1, 1)))
    return padded[:, 2:, 1:-1] + padded[:, :-2, 1:-1] + padded[:, 1:-1, 2:] + padded[:, 1:-1, :-2]


def reference(resid, basis):
    steps = resid.shape[1]
    coupling = 16.0 / (steps * steps)
    index = jnp.arange(steps).astype(jnp.float32)
    gamma = jnp.power(jnp.float32(ALPHA), index / steps)
    scaled = resid * gamma[None, :, None, None]
    rhat = jnp.fft.fft(scaled, axis=1)
    base = jnp.power(jnp.float32(ALPHA), jnp.float32(1.0) / steps)
    lam = 1.0 - base * jnp.exp(-2j * jnp.pi * index / steps)
    lam = lam[:, None, None]
    right = lam * rhat[0] + rhat[1]
    denom = lam * lam + 4.0 * coupling
    uhat = right / denom
    for sweep in range(SWEEPS - 1):
        uhat = (right + coupling * neighbours(uhat)) / denom
    vhat = lam * uhat - rhat[0]
    yhat = jnp.stack([uhat, vhat])
    precond = jnp.real(jnp.fft.ifft(yhat, axis=1)) / gamma[None, :, None, None]
    earlier = jnp.pad(precond, ((0, 0), (1, 0), (0, 0), (0, 0)))[:, :-1]
    first = precond[0] - earlier[0] - precond[1]
    second = precond[1] - earlier[1] - coupling * (neighbours(precond[0]) - 4.0 * precond[0])
    image = jnp.stack([first, second])
    inner = jnp.sum(basis * image[None], axis=(1, 2, 3, 4))
    total = jnp.sum(image * image) / image.size
    gram = jnp.concatenate([inner, total[None]])
    return precond, image, gram
```

```python
import functools

import jax
import jax.numpy as jnp
import numpy as np
from jax import lax
from jax.experimental import pallas as pl
from jax.experimental.pallas import tpu as pltpu
from jax.sharding import PartitionSpec as P

SWEEPS = 4
ALPHA = 0.01
LANES = 128
SUB = 8
GROUP = SUB // 2
FIELDS = 2
MESH = pl.DeviceIdType.MESH


def coefficients(steps):
    kappa = 16.0 / (steps * steps)
    index = np.arange(steps)
    base = ALPHA ** (1.0 / steps)
    gamma = ALPHA ** (index / steps)
    lam = 1.0 - base * np.exp(-2j * np.pi * index / steps)
    den = lam * lam + 4.0 * kappa
    wave = np.exp(2j * np.pi * (np.outer(index, index) % steps) / steps)
    scale = gamma[None, :] / gamma[:, None] / steps
    out = np.zeros((SWEEPS, FIELDS, steps, FIELDS, steps))
    for s in range(SWEEPS):
        power = kappa**s / den ** (s + 1)
        for f in range(FIELDS):
            for g in range(FIELDS):
                symbol = power * lam ** (f + 1 - g)
                if f == 1 and g == 0 and s == 0:
                    symbol = symbol - 1.0
                kernel = ((wave * symbol) @ wave.conj().T).real
                out[s, f, :, g, :] = kernel * scale
    return out.reshape(SWEEPS * FIELDS * steps, FIELDS * steps)


def split_terms(matrix):
    rest = matrix.astype(np.float32)
    pieces = []
    for _ in range(3):
        piece = rest.astype(jnp.bfloat16)
        pieces.append(piece)
        rest = rest - piece.astype(np.float32)
    one, two, three = pieces
    return np.concatenate([one, two, three, one, two, one], axis=1)


def roll(value, shift, axis):
    size = value.shape[axis]
    if isinstance(shift, int):
        shift = shift % size
        if shift == 0:
            return value
    else:
        shift = lax.rem(shift + 2 * size, size)
    return pltpu.roll(value, shift, axis)


def kernel(steps, ranks, cols, krylov, x_hbm, b_hbm, c_hbm, z_ref, im_ref, gram_ref,
           x_ref, b_ref, c_ref, pack_own, pack_halo, pack_basis, got_own, got_halo, got_basis,
           pack_out, got_out, part, parts, in_sem, send_sem, recv_sem):
    me = lax.axis_index("tm")
    row = lax.axis_index("rows")
    other = 1 - row
    width = cols // steps
    span = width + 2 * SWEEPS
    slot = LANES // 4
    kappa = 16.0 / (steps * steps)
    planes = krylov * FIELDS
    tiles = planes // 4
    lane = lax.broadcasted_iota(jnp.int32, (SUB, LANES), 1)
    sub = lax.broadcasted_iota(jnp.int32, (SUB, LANES), 0)

    barrier = pltpu.get_barrier_semaphore()

    def greet(k, carry):
        to = lax.rem(me + k, steps)
        pl.semaphore_signal(barrier, inc=1, device_id={"tm": to, "rows": row}, device_id_type=MESH)
        pl.semaphore_signal(barrier, inc=1, device_id={"tm": to, "rows": other}, device_id_type=MESH)
        return carry

    loads = [
        pltpu.make_async_copy(x_hbm, x_ref, in_sem.at[0]),
        pltpu.make_async_copy(b_hbm, b_ref, in_sem.at[1]),
        pltpu.make_async_copy(c_hbm, c_ref, in_sem.at[2]),
    ]
    for load in loads:
        load.start()
    pl.semaphore_signal(barrier, inc=1, device_id={"tm": me, "rows": other}, device_id_type=MESH)
    lax.fori_loop(1, steps, greet, 0)

    def window(read, start, count, place):
        first = max(start, 0)
        last = min(start + count, cols)
        lo = first // LANES
        hi = (last - 1) // LANES
        shift = place - start
        at = lane - place
        value = jnp.zeros((SUB, LANES), jnp.float32)
        for tile in range(lo, hi + 1):
            left = max(first, tile * LANES) - start
            right = min(last, (tile + 1) * LANES) - start
            moved = roll(read(tile), shift + tile * LANES, 1)
            value = jnp.where((at >= left) & (at < right), moved, value)
        return value

    loads[0].wait()
    lows, highs, edges = [], [], []
    for tile in range(cols // LANES):
        at = slice(tile * LANES, (tile + 1) * LANES)
        f0, f1 = x_ref[0, :, at], x_ref[1, :, at]
        low = jnp.where(sub < GROUP, f0, roll(f1, GROUP, 0))
        high = jnp.where(sub < GROUP, roll(f0, GROUP, 0), f1)
        lows.append(low)
        highs.append(high)
        edges.append(jnp.where(row == 0, high, low))
    for to in range(steps):
        start = to * width - SWEEPS
        own = window(lambda i: lows[i], start, span, span * row)
        own = own + window(lambda i: highs[i], start, span, span * (row + 1))
        pack_own[to * SUB:(to + 1) * SUB, :] = own
        pack_halo[to * SUB:(to + 1) * SUB, :] = window(lambda i: edges[i], start, span, 2 * span * row)
    loads[1].wait()
    for to in range(steps):
        for b in range(tiles):
            value = jnp.zeros((SUB, LANES), jnp.float32)
            for m in range(4):
                plane = b * 4 + m
                read = lambda i, plane=plane: b_ref[plane // FIELDS, plane % FIELDS, :, i * LANES:(i + 1) * LANES]
                value = value + window(read, to * width, width, m * slot)
            at = (to * tiles + b) * SUB
            pack_basis[at:at + SUB, :] = value

    def block(index, size):
        return pl.ds(pl.multiple_of(index * size, size), size)

    def remote(source, target, size, to, to_row, which):
        return pltpu.make_async_remote_copy(
            src_ref=source.at[block(to, size)],
            dst_ref=target.at[block(me, size)],
            send_sem=send_sem.at[which],
            recv_sem=recv_sem.at[which],
            device_id={"tm": to, "rows": to_row},
            device_id_type=MESH,
        )

    def keep(source, target, size, which):
        pltpu.make_async_copy(source.at[block(me, size)], target.at[block(me, size)], recv_sem.at[which]).start()

    def arrived(target, which):
        pltpu.make_async_copy(target, target, recv_sem.at[which]).wait()

    def left(source, count, which):
        ref = source.at[pl.ds(0, count)]
        pltpu.make_async_copy(ref, ref, send_sem.at[which]).wait()

    pl.semaphore_wait(barrier, steps * ranks - 1)

    def send_resid(k, carry):
        to = lax.rem(me + k, steps)
        remote(pack_own, got_own, SUB, to, row, 0).start()
        remote(pack_halo, got_halo, SUB, to, other, 1).start()
        return carry

    def send_basis(k, carry):
        remote(pack_basis, got_basis, SUB * tiles, lax.rem(me + k, steps), row, 2).start()
        return carry

    lax.fori_loop(1, steps, send_resid, 0)
    remote(pack_halo, got_halo, SUB, me, other, 1).start()
    keep(pack_own, got_own, SUB, 0)
    lax.fori_loop(1, steps, send_basis, 0)
    keep(pack_basis, got_basis, SUB * tiles, 2)
    loads[2].wait()

    arrived(got_own, 0)
    arrived(got_halo, 1)
    stripes = []
    for p in range(GROUP):
        pair = []
        for f in range(FIELDS):
            at = pl.ds(f * GROUP + p, steps, stride=SUB)
            pair.append(got_own[at, :] + got_halo[at, :])
        stripes.append(jnp.concatenate(pair, axis=0))
    data = jnp.concatenate(stripes, axis=1)
    one = data.astype(jnp.bfloat16)
    rest = data - one.astype(jnp.float32)
    two = rest.astype(jnp.bfloat16)
    three = (rest - two.astype(jnp.float32)).astype(jnp.bfloat16)
    stacked = jnp.concatenate([one, one, one, two, two, three], axis=0)
    depth = FIELDS * steps

    lane2 = lax.broadcasted_iota(jnp.int32, (depth, LANES), 1)
    column = lax.rem(lane2, span) + (me * width - SWEEPS)
    inside = (column >= 0) & (column < cols) & (lane2 < 3 * span)

    def term(s):
        product = jnp.dot(c_ref[s * depth:(s + 1) * depth, :], stacked, preferred_element_type=jnp.float32)
        return [product[:, p * LANES:(p + 1) * LANES] for p in range(GROUP)]

    def near(field):
        at = lane2[: field[0].shape[0]]
        out = []
        for p in range(GROUP):
            if p > 0:
                above = field[p - 1]
            else:
                above = jnp.where(at >= span, roll(field[GROUP - 1], span, 1), 0.0)
            if p < GROUP - 1:
                below = field[p + 1]
            else:
                below = jnp.where(at < 2 * span, roll(field[0], -span, 1), 0.0)
            out.append((above + below) + (roll(field[p], 1, 1) + roll(field[p], -1, 1)))
        return out

    field = term(SWEEPS - 1)
    for s in range(SWEEPS - 2, -1, -1):
        field = [a + jnp.where(inside, b, 0.0) for a, b in zip(term(s), near(field))]

    disp = [v[:steps] for v in field]
    vel = [v[steps:] for v in field]
    later = lax.broadcasted_iota(jnp.int32, (steps, LANES), 0) > 0
    before = lambda v: jnp.where(later, roll(v, 1, 0), 0.0)
    around = near(disp)
    lane1 = lane2[:steps]
    rows_out = [None] * SUB
    for p in range(GROUP):
        first = disp[p] - before(disp[p]) - vel[p]
        second = vel[p] - before(vel[p]) - kappa * (around[p] - 4.0 * disp[p])
        for h in range(2):
            value = jnp.zeros((steps, LANES), jnp.float32)
            for m, comp in enumerate((disp[p], vel[p], first, second)):
                moved = roll(comp, m * slot - SWEEPS - span * (row + h), 1)
                value = jnp.where((lane1 >= m * slot) & (lane1 < m * slot + width), moved, value)
            q = h * GROUP + p
            rows_out[q] = value
            pack_out[pl.ds(q, steps, stride=SUB), :] = value

    def send_out(k, carry):
        remote(pack_out, got_out, SUB, lax.rem(me + k, steps), row, 3).start()
        return carry

    lax.fori_loop(1, steps, send_out, 0)
    keep(pack_out, got_out, SUB, 3)

    arrived(got_basis, 2)
    sums = [jnp.zeros((steps, LANES), jnp.float32) for _ in range(tiles + 1)]
    for q in range(SUB):
        value = rows_out[q]
        twice = jnp.where(lane1 < 2 * slot, roll(value, 2 * slot, 1), value)
        for b in range(tiles):
            sums[b] = sums[b] + twice * got_basis[pl.ds(b * SUB + q, steps, stride=SUB * tiles), :]
        sums[tiles] = sums[tiles] + twice * twice
    lane0 = lax.broadcasted_iota(jnp.int32, (1, LANES), 1)
    line = jnp.zeros((1, LANES), jnp.float32)
    total = 2.0 * steps * ranks * SUB * cols
    for b in range(tiles + 1):
        folded = jnp.sum(sums[b], axis=0, keepdims=True)
        if b < tiles:
            low = jnp.sum(jnp.where(lane0 < 2 * slot, folded, 0.0), axis=1, keepdims=True)
            high = jnp.sum(jnp.where(lane0 >= 2 * slot, folded, 0.0), axis=1, keepdims=True)
            line = jnp.where(lane0 == 2 * b, low, jnp.where(lane0 == 2 * b + 1, high, line))
        else:
            low = jnp.sum(jnp.where(lane0 < 2 * slot, folded, 0.0), axis=1, keepdims=True)
            line = jnp.where(lane0 == krylov, low * (1.0 / total), line)
    part[...] = line[None]
    mine = me * ranks + row

    def tell(to, to_row):
        pltpu.make_async_remote_copy(
            src_ref=part,
            dst_ref=parts.at[pl.ds(mine, 1)],
            send_sem=send_sem.at[4],
            recv_sem=recv_sem.at[4],
            device_id={"tm": to, "rows": to_row},
            device_id_type=MESH,
        ).start()

    def send_part(k, carry):
        to = lax.rem(me + k, steps)
        tell(to, row)
        tell(to, other)
        return carry

    lax.fori_loop(1, steps, send_part, 0)
    tell(me, other)
    pltpu.make_async_copy(part, parts.at[pl.ds(mine, 1)], recv_sem.at[4]).start()

    arrived(got_out, 3)
    per = LANES // width
    for tile in range(cols // LANES):
        values = [jnp.zeros((SUB, LANES), jnp.float32) for _ in range(4)]
        for i in range(per):
            source = tile * per + i
            got = got_out[source * SUB:(source + 1) * SUB, :]
            spot = (lane >= i * width) & (lane < (i + 1) * width)
            for m in range(4):
                values[m] = jnp.where(spot, roll(got, i * width - m * slot, 1), values[m])
        at = slice(tile * LANES, (tile + 1) * LANES)
        z_ref[0, :, at] = values[0]
        z_ref[1, :, at] = values[1]
        im_ref[0, :, at] = values[2]
        im_ref[1, :, at] = values[3]

    arrived(parts, 4)
    gram_ref[...] = jnp.sum(parts[...], axis=0)
    left(pack_own, (steps - 1) * SUB, 0)
    left(pack_halo, steps * SUB, 1)
    left(pack_basis, (steps - 1) * SUB * tiles, 2)
    left(pack_out, (steps - 1) * SUB, 3)
    left(parts, steps * ranks - 1, 4)


def solution(mesh):
    steps, ranks = mesh.shape["tm"], mesh.shape["rows"]
    table = split_terms(coefficients(steps))

    def on_device(resid, basis):
        rows_dev, cols = resid.shape[2:]
        krylov = basis.shape[0]
        width = cols // steps
        assert ranks == 2 and rows_dev == SUB and cols % LANES == 0 and cols % steps == 0
        assert LANES % width == 0 and 4 * width <= LANES and 3 * (width + 2 * SWEEPS) <= LANES
        assert (krylov * FIELDS) % 4 == 0 and steps % SUB == 0
        tiles = krylov * FIELDS // 4
        const = jnp.asarray(table)
        vmem = lambda *shape: pltpu.VMEM(shape, jnp.float32)
        plane = jax.ShapeDtypeStruct((FIELDS, rows_dev, cols), jnp.float32)
        z, image, gram = pl.pallas_call(
            functools.partial(kernel, steps, ranks, cols, krylov),
            out_shape=[plane, plane, jax.ShapeDtypeStruct((1, LANES), jnp.float32)],
            in_specs=[pl.BlockSpec(memory_space=pl.ANY)] * 3,
            out_specs=[pl.BlockSpec(memory_space=pltpu.VMEM)] * 3,
            scratch_shapes=[
                vmem(FIELDS, rows_dev, cols),
                vmem(krylov, FIELDS, rows_dev, cols),
                pltpu.VMEM(table.shape, jnp.bfloat16),
                vmem(steps * SUB, LANES),
                vmem(steps * SUB, LANES),
                vmem(steps * SUB * tiles, LANES),
                vmem(steps * SUB, LANES),
                vmem(steps * SUB, LANES),
                vmem(steps * SUB * tiles, LANES),
                vmem(steps * SUB, LANES),
                vmem(steps * SUB, LANES),
                vmem(1, 1, LANES),
                vmem(steps * ranks, 1, LANES),
                pltpu.SemaphoreType.DMA((3,)),
                pltpu.SemaphoreType.DMA((5,)),
                pltpu.SemaphoreType.DMA((5,)),
            ],
            compiler_params=pltpu.CompilerParams(collective_id=0, has_side_effects=True),
        )(resid[:, 0], basis[:, :, 0], const)
        return z[:, None], image[:, None], gram[0, : krylov + 1]

    return jax.shard_map(
        on_device,
        mesh=mesh,
        in_specs=(P(None, "tm", "rows", None), P(None, None, "tm", "rows", None)),
        out_specs=(P(None, "tm", "rows", None), P(None, "tm", "rows", None), P()),
        check_vma=False,
    )
```

```python
import functools

import jax
import jax.numpy as jnp
import numpy as np
from jax import lax
from jax.experimental import pallas as pl
from jax.experimental.pallas import tpu as pltpu
from jax.sharding import PartitionSpec as P

SWEEPS = 4
ALPHA = 0.01
LANES = 128
SUB = 8
GROUP = SUB // 2
FIELDS = 2
MESH = pl.DeviceIdType.MESH


def coefficients(steps):
    kappa = 16.0 / (steps * steps)
    index = np.arange(steps)
    base = ALPHA ** (1.0 / steps)
    gamma = ALPHA ** (index / steps)
    lam = 1.0 - base * np.exp(-2j * np.pi * index / steps)
    den = lam * lam + 4.0 * kappa
    wave = np.exp(2j * np.pi * (np.outer(index, index) % steps) / steps)
    scale = gamma[None, :] / gamma[:, None] / steps
    out = np.zeros((SWEEPS, FIELDS, steps, FIELDS, steps))
    for s in range(SWEEPS):
        power = kappa**s / den ** (s + 1)
        for f in range(FIELDS):
            for g in range(FIELDS):
                symbol = power * lam ** (f + 1 - g)
                if f == 1 and g == 0 and s == 0:
                    symbol = symbol - 1.0
                kernel = ((wave * symbol) @ wave.conj().T).real
                out[s, f, :, g, :] = kernel * scale
    return out.reshape(SWEEPS * FIELDS * steps, FIELDS * steps)


def split_terms(matrix):
    rest = matrix.astype(np.float32)
    pieces = []
    for _ in range(3):
        piece = rest.astype(jnp.bfloat16)
        pieces.append(piece)
        rest = rest - piece.astype(np.float32)
    one, two, three = pieces
    return np.concatenate([one, two, three, one, two, one], axis=1)


def roll(value, shift, axis):
    size = value.shape[axis]
    if isinstance(shift, int):
        shift = shift % size
        if shift == 0:
            return value
    else:
        shift = lax.rem(shift + 2 * size, size)
    return pltpu.roll(value, shift, axis)


def unpack(steps, krylov, got_out, parts, z_ref, im_ref, gram_ref):
    cols = z_ref.shape[2]
    width = cols // steps
    slot = LANES // 4
    per = LANES // width
    lane = lax.broadcasted_iota(jnp.int32, (SUB, LANES), 1)
    for tile in range(cols // LANES):
        values = [jnp.zeros((SUB, LANES), jnp.float32) for _ in range(4)]
        for i in range(per):
            source = tile * per + i
            got = got_out[source * SUB:(source + 1) * SUB, :]
            spot = (lane >= i * width) & (lane < (i + 1) * width)
            for m in range(4):
                values[m] = jnp.where(spot, roll(got, i * width - m * slot, 1), values[m])
        at = slice(tile * LANES, (tile + 1) * LANES)
        z_ref[0, :, at] = values[0]
        z_ref[1, :, at] = values[1]
        im_ref[0, :, at] = values[2]
        im_ref[1, :, at] = values[3]
    gram_ref[...] = jnp.sum(parts[...], axis=(0, 1))[: krylov + 1]


def kernel(steps, ranks, cols, krylov, x_hbm, b_hbm, c_hbm, got_out, parts,
           x_ref, b_ref, c_ref, pack_own, pack_halo, pack_basis, got_own, got_halo, got_basis,
           pack_out, part, in_sem, send_sem, recv_sem):
    me = lax.axis_index("tm")
    row = lax.axis_index("rows")
    other = 1 - row
    width = cols // steps
    span = width + 2 * SWEEPS
    slot = LANES // 4
    kappa = 16.0 / (steps * steps)
    planes = krylov * FIELDS
    tiles = planes // 4
    lane = lax.broadcasted_iota(jnp.int32, (SUB, LANES), 1)
    sub = lax.broadcasted_iota(jnp.int32, (SUB, LANES), 0)

    barrier = pltpu.get_barrier_semaphore()

    def greet(k, carry):
        to = lax.rem(me + k, steps)
        pl.semaphore_signal(barrier, inc=1, device_id={"tm": to, "rows": row}, device_id_type=MESH)
        pl.semaphore_signal(barrier, inc=1, device_id={"tm": to, "rows": other}, device_id_type=MESH)
        return carry

    loads = [
        pltpu.make_async_copy(x_hbm, x_ref, in_sem.at[0]),
        pltpu.make_async_copy(b_hbm, b_ref, in_sem.at[1]),
        pltpu.make_async_copy(c_hbm, c_ref, in_sem.at[2]),
    ]
    for load in loads:
        load.start()
    pl.semaphore_signal(barrier, inc=1, device_id={"tm": me, "rows": other}, device_id_type=MESH)
    lax.fori_loop(1, steps, greet, 0)

    def window(read, start, count, place):
        first = max(start, 0)
        last = min(start + count, cols)
        lo = first // LANES
        hi = (last - 1) // LANES
        shift = place - start
        at = lane - place
        value = jnp.zeros((SUB, LANES), jnp.float32)
        for tile in range(lo, hi + 1):
            left = max(first, tile * LANES) - start
            right = min(last, (tile + 1) * LANES) - start
            moved = roll(read(tile), shift + tile * LANES, 1)
            value = jnp.where((at >= left) & (at < right), moved, value)
        return value

    loads[0].wait()
    lows, highs, edges = [], [], []
    for tile in range(cols // LANES):
        at = slice(tile * LANES, (tile + 1) * LANES)
        f0, f1 = x_ref[0, :, at], x_ref[1, :, at]
        low = jnp.where(sub < GROUP, f0, roll(f1, GROUP, 0))
        high = jnp.where(sub < GROUP, roll(f0, GROUP, 0), f1)
        lows.append(low)
        highs.append(high)
        edges.append(jnp.where(row == 0, high, low))
    for to in range(steps):
        start = to * width - SWEEPS
        own = window(lambda i: lows[i], start, span, span * row)
        own = own + window(lambda i: highs[i], start, span, span * (row + 1))
        pack_own[to * SUB:(to + 1) * SUB, :] = own
        pack_halo[to * SUB:(to + 1) * SUB, :] = window(lambda i: edges[i], start, span, 2 * span * row)
    def block(index, size):
        return pl.ds(pl.multiple_of(index * size, size), size)

    def remote(source, target, size, to, to_row, which):
        return pltpu.make_async_remote_copy(
            src_ref=source.at[block(to, size)],
            dst_ref=target.at[block(me, size)],
            send_sem=send_sem.at[which],
            recv_sem=recv_sem.at[which],
            device_id={"tm": to, "rows": to_row},
            device_id_type=MESH,
        )

    def keep(source, target, size, which):
        pltpu.make_async_copy(source.at[block(me, size)], target.at[block(me, size)], recv_sem.at[which]).start()

    def arrived(target, which):
        pltpu.make_async_copy(target, target, recv_sem.at[which]).wait()

    def left(source, count, which):
        ref = source.at[pl.ds(0, count)]
        pltpu.make_async_copy(ref, ref, send_sem.at[which]).wait()

    pl.semaphore_wait(barrier, steps * ranks - 1)

    def send_resid(k, carry):
        to = lax.rem(me + k, steps)
        remote(pack_own, got_own, SUB, to, row, 0).start()
        remote(pack_halo, got_halo, SUB, to, other, 1).start()
        return carry

    def send_basis(k, carry):
        remote(pack_basis, got_basis, SUB * tiles, lax.rem(me + k, steps), row, 2).start()
        return carry

    lax.fori_loop(1, steps, send_resid, 0)
    remote(pack_halo, got_halo, SUB, me, other, 1).start()
    keep(pack_own, got_own, SUB, 0)

    loads[1].wait()
    for to in range(steps):
        for b in range(tiles):
            value = jnp.zeros((SUB, LANES), jnp.float32)
            for m in range(4):
                plane = b * 4 + m
                read = lambda i, plane=plane: b_ref[plane // FIELDS, plane % FIELDS, :, i * LANES:(i + 1) * LANES]
                value = value + window(read, to * width, width, m * slot)
            at = (to * tiles + b) * SUB
            pack_basis[at:at + SUB, :] = value
    lax.fori_loop(1, steps, send_basis, 0)
    keep(pack_basis, got_basis, SUB * tiles, 2)
    loads[2].wait()

    arrived(got_own, 0)
    arrived(got_halo, 1)
    stripes = []
    for p in range(GROUP):
        pair = []
        for f in range(FIELDS):
            at = pl.ds(f * GROUP + p, steps, stride=SUB)
            pair.append(got_own[at, :] + got_halo[at, :])
        stripes.append(jnp.concatenate(pair, axis=0))
    data = jnp.concatenate(stripes, axis=1)
    one = data.astype(jnp.bfloat16)
    rest = data - one.astype(jnp.float32)
    two = rest.astype(jnp.bfloat16)
    three = (rest - two.astype(jnp.float32)).astype(jnp.bfloat16)
    stacked = jnp.concatenate([one, one, one, two, two, three], axis=0)
    depth = FIELDS * steps

    lane2 = lax.broadcasted_iota(jnp.int32, (depth, LANES), 1)
    column = lax.rem(lane2, span) + (me * width - SWEEPS)
    inside = (column >= 0) & (column < cols) & (lane2 < 3 * span)

    def term(s):
        product = jnp.dot(c_ref[s * depth:(s + 1) * depth, :], stacked, preferred_element_type=jnp.float32)
        return [product[:, p * LANES:(p + 1) * LANES] for p in range(GROUP)]

    def near(field):
        at = lane2[: field[0].shape[0]]
        out = []
        for p in range(GROUP):
            if p > 0:
                above = field[p - 1]
            else:
                above = jnp.where(at >= span, roll(field[GROUP - 1], span, 1), 0.0)
            if p < GROUP - 1:
                below = field[p + 1]
            else:
                below = jnp.where(at < 2 * span, roll(field[0], -span, 1), 0.0)
            out.append((above + below) + (roll(field[p], 1, 1) + roll(field[p], -1, 1)))
        return out

    field = term(SWEEPS - 1)
    for s in range(SWEEPS - 2, -1, -1):
        field = [a + jnp.where(inside, b, 0.0) for a, b in zip(term(s), near(field))]

    disp = [v[:steps] for v in field]
    vel = [v[steps:] for v in field]
    later = lax.broadcasted_iota(jnp.int32, (steps, LANES), 0) > 0
    before = lambda v: jnp.where(later, roll(v, 1, 0), 0.0)
    around = near(disp)
    lane1 = lane2[:steps]
    rows_out = [None] * SUB
    for p in range(GROUP):
        first = disp[p] - before(disp[p]) - vel[p]
        second = vel[p] - before(vel[p]) - kappa * (around[p] - 4.0 * disp[p])
        for h in range(2):
            value = jnp.zeros((steps, LANES), jnp.float32)
            for m, comp in enumerate((disp[p], vel[p], first, second)):
                moved = roll(comp, m * slot - SWEEPS - span * (row + h), 1)
                value = jnp.where((lane1 >= m * slot) & (lane1 < m * slot + width), moved, value)
            q = h * GROUP + p
            rows_out[q] = value
            pack_out[pl.ds(q, steps, stride=SUB), :] = value

    def send_out(k, carry):
        remote(pack_out, got_out, SUB, lax.rem(me + k, steps), row, 3).start()
        return carry

    lax.fori_loop(1, steps, send_out, 0)
    keep(pack_out, got_out, SUB, 3)

    arrived(got_basis, 2)
    sums = [jnp.zeros((steps, LANES), jnp.float32) for _ in range(tiles + 1)]
    for q in range(SUB):
        value = rows_out[q]
        twice = jnp.where(lane1 < 2 * slot, roll(value, 2 * slot, 1), value)
        for b in range(tiles):
            sums[b] = sums[b] + twice * got_basis[pl.ds(b * SUB + q, steps, stride=SUB * tiles), :]
        sums[tiles] = sums[tiles] + twice * twice
    lane0 = lax.broadcasted_iota(jnp.int32, (1, LANES), 1)
    line = jnp.zeros((1, LANES), jnp.float32)
    total = 2.0 * steps * ranks * SUB * cols
    for b in range(tiles + 1):
        folded = jnp.sum(sums[b], axis=0, keepdims=True)
        if b < tiles:
            low = jnp.sum(jnp.where(lane0 < 2 * slot, folded, 0.0), axis=1, keepdims=True)
            high = jnp.sum(jnp.where(lane0 >= 2 * slot, folded, 0.0), axis=1, keepdims=True)
            line = jnp.where(lane0 == 2 * b, low, jnp.where(lane0 == 2 * b + 1, high, line))
        else:
            low = jnp.sum(jnp.where(lane0 < 2 * slot, folded, 0.0), axis=1, keepdims=True)
            line = jnp.where(lane0 == krylov, low * (1.0 / total), line)
    part[...] = line[None]
    mine = me * ranks + row

    def tell(to, to_row):
        pltpu.make_async_remote_copy(
            src_ref=part,
            dst_ref=parts.at[pl.ds(mine, 1)],
            send_sem=send_sem.at[4],
            recv_sem=recv_sem.at[4],
            device_id={"tm": to, "rows": to_row},
            device_id_type=MESH,
        ).start()

    def send_part(k, carry):
        to = lax.rem(me + k, steps)
        tell(to, row)
        tell(to, other)
        return carry

    lax.fori_loop(1, steps, send_part, 0)
    tell(me, other)
    pltpu.make_async_copy(part, parts.at[pl.ds(mine, 1)], recv_sem.at[4]).start()

    arrived(got_out, 3)
    arrived(parts, 4)
    left(pack_own, (steps - 1) * SUB, 0)
    left(pack_halo, steps * SUB, 1)
    left(pack_basis, (steps - 1) * SUB * tiles, 2)
    left(pack_out, (steps - 1) * SUB, 3)
    left(parts, steps * ranks - 1, 4)


def solution(mesh):
    steps, ranks = mesh.shape["tm"], mesh.shape["rows"]
    table = split_terms(coefficients(steps))

    def on_device(resid, basis):
        rows_dev, cols = resid.shape[2:]
        krylov = basis.shape[0]
        width = cols // steps
        assert ranks == 2 and rows_dev == SUB and cols % LANES == 0 and cols % steps == 0
        assert LANES % width == 0 and 4 * width <= LANES and 3 * (width + 2 * SWEEPS) <= LANES
        assert (krylov * FIELDS) % 4 == 0 and steps % SUB == 0
        tiles = krylov * FIELDS // 4
        const = jnp.asarray(table)
        limit = 32 * 1024 * 1024
        vmem = lambda *shape: pltpu.VMEM(shape, jnp.float32)
        plane = jax.ShapeDtypeStruct((FIELDS, rows_dev, cols), jnp.float32)
        got, parts = pl.pallas_call(
            functools.partial(kernel, steps, ranks, cols, krylov),
            out_shape=[
                jax.ShapeDtypeStruct((steps * SUB, LANES), jnp.float32),
                jax.ShapeDtypeStruct((steps * ranks, 1, LANES), jnp.float32),
            ],
            in_specs=[pl.BlockSpec(memory_space=pltpu.HBM)] * 3,
            out_specs=[pl.BlockSpec(memory_space=pl.ANY)] * 2,
            scratch_shapes=[
                vmem(FIELDS, rows_dev, cols),
                vmem(krylov, FIELDS, rows_dev, cols),
                pltpu.VMEM(table.shape, jnp.bfloat16),
                vmem(steps * SUB, LANES),
                vmem(steps * SUB, LANES),
                vmem(steps * SUB * tiles, LANES),
                vmem(steps * SUB, LANES),
                vmem(steps * SUB, LANES),
                vmem(steps * SUB * tiles, LANES),
                vmem(steps * SUB, LANES),
                vmem(1, 1, LANES),
                pltpu.SemaphoreType.DMA((3,)),
                pltpu.SemaphoreType.DMA((5,)),
                pltpu.SemaphoreType.DMA((5,)),
            ],
            compiler_params=pltpu.CompilerParams(collective_id=0, has_side_effects=True, vmem_limit_bytes=limit),
        )(resid[:, 0], basis[:, :, 0], const)
        z, image, gram = pl.pallas_call(
            functools.partial(unpack, steps, krylov),
            out_shape=[plane, plane, jax.ShapeDtypeStruct((krylov + 1,), jnp.float32)],
            in_specs=[pl.BlockSpec(memory_space=pltpu.VMEM)] * 2,
            out_specs=[pl.BlockSpec(memory_space=pltpu.VMEM)] * 3,
            compiler_params=pltpu.CompilerParams(vmem_limit_bytes=limit),
        )(got, parts)
        return z[:, None], image[:, None], gram

    return jax.shard_map(
        on_device,
        mesh=mesh,
        in_specs=(P(None, "tm", "rows", None), P(None, None, "tm", "rows", None)),
        out_specs=(P(None, "tm", "rows", None), P(None, "tm", "rows", None), P()),
        check_vma=False,
    )
```

```python
import functools

import jax
import jax.numpy as jnp
import numpy as np
from jax import lax
from jax.experimental import pallas as pl
from jax.experimental.pallas import tpu as pltpu
from jax.sharding import PartitionSpec as P

SWEEPS = 4
ALPHA = 0.01
LANES = 128
SUB = 8
GROUP = SUB // 2
FIELDS = 2
MESH = pl.DeviceIdType.MESH


def coefficients(steps):
    kappa = 16.0 / (steps * steps)
    index = np.arange(steps)
    base = ALPHA ** (1.0 / steps)
    gamma = ALPHA ** (index / steps)
    lam = 1.0 - base * np.exp(-2j * np.pi * index / steps)
    den = lam * lam + 4.0 * kappa
    wave = np.exp(2j * np.pi * (np.outer(index, index) % steps) / steps)
    scale = gamma[None, :] / gamma[:, None] / steps
    out = np.zeros((SWEEPS, FIELDS, steps, FIELDS, steps))
    for s in range(SWEEPS):
        power = kappa**s / den ** (s + 1)
        for f in range(FIELDS):
            for g in range(FIELDS):
                symbol = power * lam ** (f + 1 - g)
                if f == 1 and g == 0 and s == 0:
                    symbol = symbol - 1.0
                kernel = ((wave * symbol) @ wave.conj().T).real
                out[s, f, :, g, :] = kernel * scale
    return out.reshape(SWEEPS * FIELDS * steps, FIELDS * steps)


def split_terms(matrix):
    rest = matrix.astype(np.float32)
    pieces = []
    for _ in range(3):
        piece = rest.astype(jnp.bfloat16)
        pieces.append(piece)
        rest = rest - piece.astype(np.float32)
    one, two, three = pieces
    return np.concatenate([one, two, three, one, two, one], axis=1)


def roll(value, shift, axis):
    size = value.shape[axis]
    if isinstance(shift, int):
        shift = shift % size
        if shift == 0:
            return value
    else:
        shift = lax.rem(shift + 2 * size, size)
    return pltpu.roll(value, shift, axis)


def unpack(steps, krylov, got_out, parts, z_ref, im_ref, gram_ref):
    cols = z_ref.shape[2]
    width = cols // steps
    slot = LANES // 4
    per = LANES // width
    lane = lax.broadcasted_iota(jnp.int32, (SUB, LANES), 1)
    for tile in range(cols // LANES):
        values = [jnp.zeros((SUB, LANES), jnp.float32) for _ in range(4)]
        for i in range(per):
            source = tile * per + i
            got = got_out[source * SUB:(source + 1) * SUB, :]
            spot = (lane >= i * width) & (lane < (i + 1) * width)
            for m in range(4):
                values[m] = jnp.where(spot, roll(got, i * width - m * slot, 1), values[m])
        at = slice(tile * LANES, (tile + 1) * LANES)
        z_ref[0, :, at] = values[0]
        z_ref[1, :, at] = values[1]
        im_ref[0, :, at] = values[2]
        im_ref[1, :, at] = values[3]
    gram_ref[...] = jnp.sum(parts[...], axis=(0, 1))[: krylov + 1]


def kernel(steps, ranks, cols, krylov, x_hbm, b_hbm, c_hbm, got_out, parts,
           x_ref, b_ref, c_ref, pack_own, pack_halo, pack_basis, got_own, got_halo, got_basis,
           pack_out, part, in_sem, send_sem, recv_sem):
    me = lax.axis_index("tm")
    row = lax.axis_index("rows")
    other = 1 - row
    width = cols // steps
    span = width + 2 * SWEEPS
    slot = LANES // 4
    kappa = 16.0 / (steps * steps)
    planes = krylov * FIELDS
    tiles = planes // 4
    lane = lax.broadcasted_iota(jnp.int32, (SUB, LANES), 1)
    sub = lax.broadcasted_iota(jnp.int32, (SUB, LANES), 0)

    barrier = pltpu.get_barrier_semaphore()

    def peer(k):
        return lax.rem(me + lax.rem(k + steps // 2 - 2, steps - 1) + 1, steps)

    def greet(k, carry):
        to = peer(k)
        pl.semaphore_signal(barrier, inc=1, device_id={"tm": to, "rows": row}, device_id_type=MESH)
        pl.semaphore_signal(barrier, inc=1, device_id={"tm": to, "rows": other}, device_id_type=MESH)
        return carry

    loads = [
        pltpu.make_async_copy(x_hbm, x_ref, in_sem.at[0]),
        pltpu.make_async_copy(b_hbm, b_ref, in_sem.at[1]),
        pltpu.make_async_copy(c_hbm, c_ref, in_sem.at[2]),
    ]
    for load in loads:
        load.start()
    pl.semaphore_signal(barrier, inc=1, device_id={"tm": me, "rows": other}, device_id_type=MESH)
    lax.fori_loop(1, steps, greet, 0)

    def window(read, start, count, place):
        first = max(start, 0)
        last = min(start + count, cols)
        lo = first // LANES
        hi = (last - 1) // LANES
        shift = place - start
        at = lane - place
        value = jnp.zeros((SUB, LANES), jnp.float32)
        for tile in range(lo, hi + 1):
            left = max(first, tile * LANES) - start
            right = min(last, (tile + 1) * LANES) - start
            moved = roll(read(tile), shift + tile * LANES, 1)
            value = jnp.where((at >= left) & (at < right), moved, value)
        return value

    loads[0].wait()
    lows, highs, edges = [], [], []
    for tile in range(cols // LANES):
        at = slice(tile * LANES, (tile + 1) * LANES)
        f0, f1 = x_ref[0, :, at], x_ref[1, :, at]
        low = jnp.where(sub < GROUP, f0, roll(f1, GROUP, 0))
        high = jnp.where(sub < GROUP, roll(f0, GROUP, 0), f1)
        lows.append(low)
        highs.append(high)
        edges.append(jnp.where(row == 0, high, low))
    for to in range(steps):
        start = to * width - SWEEPS
        own = window(lambda i: lows[i], start, span, span * row)
        own = own + window(lambda i: highs[i], start, span, span * (row + 1))
        pack_own[to * SUB:(to + 1) * SUB, :] = own
        pack_halo[to * SUB:(to + 1) * SUB, :] = window(lambda i: edges[i], start, span, 2 * span * row)
    def block(index, size):
        return pl.ds(pl.multiple_of(index * size, size), size)

    def remote(source, target, size, to, to_row, which):
        return pltpu.make_async_remote_copy(
            src_ref=source.at[block(to, size)],
            dst_ref=target.at[block(me, size)],
            send_sem=send_sem.at[which],
            recv_sem=recv_sem.at[which],
            device_id={"tm": to, "rows": to_row},
            device_id_type=MESH,
        )

    def keep(source, target, size, which):
        pltpu.make_async_copy(source.at[block(me, size)], target.at[block(me, size)], recv_sem.at[which]).start()

    def arrived(target, which):
        pltpu.make_async_copy(target, target, recv_sem.at[which]).wait()

    def left(source, count, which):
        ref = source.at[pl.ds(0, count)]
        pltpu.make_async_copy(ref, ref, send_sem.at[which]).wait()

    pl.semaphore_wait(barrier, steps * ranks - 1)

    def send_resid(k, carry):
        to = peer(k)
        remote(pack_own, got_own, SUB, to, row, 0).start()
        remote(pack_halo, got_halo, SUB, to, other, 1).start()
        return carry

    def send_basis(k, carry):
        remote(pack_basis, got_basis, SUB * tiles, peer(k), row, 2).start()
        return carry

    lax.fori_loop(1, steps, send_resid, 0)
    remote(pack_halo, got_halo, SUB, me, other, 1).start()
    keep(pack_own, got_own, SUB, 0)

    loads[1].wait()
    for to in range(steps):
        for b in range(tiles):
            value = jnp.zeros((SUB, LANES), jnp.float32)
            for m in range(4):
                plane = b * 4 + m
                read = lambda i, plane=plane: b_ref[plane // FIELDS, plane % FIELDS, :, i * LANES:(i + 1) * LANES]
                value = value + window(read, to * width, width, m * slot)
            at = (to * tiles + b) * SUB
            pack_basis[at:at + SUB, :] = value
    lax.fori_loop(1, steps, send_basis, 0)
    keep(pack_basis, got_basis, SUB * tiles, 2)
    loads[2].wait()

    arrived(got_own, 0)
    arrived(got_halo, 1)
    stripes = []
    for p in range(GROUP):
        pair = []
        for f in range(FIELDS):
            at = pl.ds(f * GROUP + p, steps, stride=SUB)
            pair.append(got_own[at, :] + got_halo[at, :])
        stripes.append(jnp.concatenate(pair, axis=0))
    data = jnp.concatenate(stripes, axis=1)
    one = data.astype(jnp.bfloat16)
    rest = data - one.astype(jnp.float32)
    two = rest.astype(jnp.bfloat16)
    three = (rest - two.astype(jnp.float32)).astype(jnp.bfloat16)
    stacked = jnp.concatenate([one, one, one, two, two, three], axis=0)
    depth = FIELDS * steps

    lane2 = lax.broadcasted_iota(jnp.int32, (depth, LANES), 1)
    column = lax.rem(lane2, span) + (me * width - SWEEPS)
    inside = (column >= 0) & (column < cols) & (lane2 < 3 * span)

    def term(s):
        product = jnp.dot(c_ref[s * depth:(s + 1) * depth, :], stacked, preferred_element_type=jnp.float32)
        return [product[:, p * LANES:(p + 1) * LANES] for p in range(GROUP)]

    def near(field):
        at = lane2[: field[0].shape[0]]
        out = []
        for p in range(GROUP):
            if p > 0:
                above = field[p - 1]
            else:
                above = jnp.where(at >= span, roll(field[GROUP - 1], span, 1), 0.0)
            if p < GROUP - 1:
                below = field[p + 1]
            else:
                below = jnp.where(at < 2 * span, roll(field[0], -span, 1), 0.0)
            out.append((above + below) + (roll(field[p], 1, 1) + roll(field[p], -1, 1)))
        return out

    field = term(SWEEPS - 1)
    for s in range(SWEEPS - 2, -1, -1):
        field = [a + jnp.where(inside, b, 0.0) for a, b in zip(term(s), near(field))]

    disp = [v[:steps] for v in field]
    vel = [v[steps:] for v in field]
    later = lax.broadcasted_iota(jnp.int32, (steps, LANES), 0) > 0
    before = lambda v: jnp.where(later, roll(v, 1, 0), 0.0)
    around = near(disp)
    lane1 = lane2[:steps]
    rows_out = [None] * SUB
    for p in range(GROUP):
        first = disp[p] - before(disp[p]) - vel[p]
        second = vel[p] - before(vel[p]) - kappa * (around[p] - 4.0 * disp[p])
        for h in range(2):
            value = jnp.zeros((steps, LANES), jnp.float32)
            for m, comp in enumerate((disp[p], vel[p], first, second)):
                moved = roll(comp, m * slot - SWEEPS - span * (row + h), 1)
                value = jnp.where((lane1 >= m * slot) & (lane1 < m * slot + width), moved, value)
            q = h * GROUP + p
            rows_out[q] = value
            pack_out[pl.ds(q, steps, stride=SUB), :] = value

    def send_out(k, carry):
        remote(pack_out, got_out, SUB, peer(k), row, 3).start()
        return carry

    lax.fori_loop(1, steps, send_out, 0)
    keep(pack_out, got_out, SUB, 3)

    arrived(got_basis, 2)
    sums = [jnp.zeros((steps, LANES), jnp.float32) for _ in range(tiles + 1)]
    for q in range(SUB):
        value = rows_out[q]
        twice = jnp.where(lane1 < 2 * slot, roll(value, 2 * slot, 1), value)
        for b in range(tiles):
            sums[b] = sums[b] + twice * got_basis[pl.ds(b * SUB + q, steps, stride=SUB * tiles), :]
        sums[tiles] = sums[tiles] + twice * twice
    lane0 = lax.broadcasted_iota(jnp.int32, (1, LANES), 1)
    line = jnp.zeros((1, LANES), jnp.float32)
    total = 2.0 * steps * ranks * SUB * cols
    for b in range(tiles + 1):
        folded = jnp.sum(sums[b], axis=0, keepdims=True)
        if b < tiles:
            low = jnp.sum(jnp.where(lane0 < 2 * slot, folded, 0.0), axis=1, keepdims=True)
            high = jnp.sum(jnp.where(lane0 >= 2 * slot, folded, 0.0), axis=1, keepdims=True)
            line = jnp.where(lane0 == 2 * b, low, jnp.where(lane0 == 2 * b + 1, high, line))
        else:
            low = jnp.sum(jnp.where(lane0 < 2 * slot, folded, 0.0), axis=1, keepdims=True)
            line = jnp.where(lane0 == krylov, low * (1.0 / total), line)
    part[...] = line[None]
    mine = me * ranks + row

    def tell(to, to_row):
        pltpu.make_async_remote_copy(
            src_ref=part,
            dst_ref=parts.at[pl.ds(mine, 1)],
            send_sem=send_sem.at[4],
            recv_sem=recv_sem.at[4],
            device_id={"tm": to, "rows": to_row},
            device_id_type=MESH,
        ).start()

    def send_part(k, carry):
        to = peer(k)
        tell(to, row)
        tell(to, other)
        return carry

    lax.fori_loop(1, steps, send_part, 0)
    tell(me, other)
    pltpu.make_async_copy(part, parts.at[pl.ds(mine, 1)], recv_sem.at[4]).start()

    arrived(got_out, 3)
    arrived(parts, 4)
    left(pack_own, (steps - 1) * SUB, 0)
    left(pack_halo, steps * SUB, 1)
    left(pack_basis, (steps - 1) * SUB * tiles, 2)
    left(pack_out, (steps - 1) * SUB, 3)
    left(parts, steps * ranks - 1, 4)


def solution(mesh):
    steps, ranks = mesh.shape["tm"], mesh.shape["rows"]
    table = split_terms(coefficients(steps))

    def on_device(resid, basis):
        rows_dev, cols = resid.shape[2:]
        krylov = basis.shape[0]
        width = cols // steps
        assert ranks == 2 and rows_dev == SUB and cols % LANES == 0 and cols % steps == 0
        assert LANES % width == 0 and 4 * width <= LANES and 3 * (width + 2 * SWEEPS) <= LANES
        assert (krylov * FIELDS) % 4 == 0 and steps % SUB == 0
        tiles = krylov * FIELDS // 4
        const = jnp.asarray(table)
        limit = 55100 * 1024
        vmem = lambda *shape: pltpu.VMEM(shape, jnp.float32)
        plane = jax.ShapeDtypeStruct((FIELDS, rows_dev, cols), jnp.float32)
        got, parts = pl.pallas_call(
            functools.partial(kernel, steps, ranks, cols, krylov),
            out_shape=[
                jax.ShapeDtypeStruct((steps * SUB, LANES), jnp.float32),
                jax.ShapeDtypeStruct((steps * ranks, 1, LANES), jnp.float32),
            ],
            in_specs=[pl.BlockSpec(memory_space=pltpu.HBM)] * 3,
            out_specs=[pl.BlockSpec(memory_space=pl.ANY)] * 2,
            scratch_shapes=[
                vmem(FIELDS, rows_dev, cols),
                vmem(krylov, FIELDS, rows_dev, cols),
                pltpu.VMEM(table.shape, jnp.bfloat16),
                vmem(steps * SUB, LANES),
                vmem(steps * SUB, LANES),
                vmem(steps * SUB * tiles, LANES),
                vmem(steps * SUB, LANES),
                vmem(steps * SUB, LANES),
                vmem(steps * SUB * tiles, LANES),
                vmem(steps * SUB, LANES),
                vmem(1, 1, LANES),
                pltpu.SemaphoreType.DMA((3,)),
                pltpu.SemaphoreType.DMA((5,)),
                pltpu.SemaphoreType.DMA((5,)),
            ],
            compiler_params=pltpu.CompilerParams(collective_id=0, has_side_effects=True, vmem_limit_bytes=limit),
        )(resid[:, 0], basis[:, :, 0], const)
        z, image, gram = pl.pallas_call(
            functools.partial(unpack, steps, krylov),
            out_shape=[plane, plane, jax.ShapeDtypeStruct((krylov + 1,), jnp.float32)],
            in_specs=[pl.BlockSpec(memory_space=pltpu.VMEM)] * 2,
            out_specs=[pl.BlockSpec(memory_space=pltpu.VMEM)] * 3,
            compiler_params=pltpu.CompilerParams(vmem_limit_bytes=32 * 1024 * 1024),
        )(got, parts)
        return z[:, None], image[:, None], gram

    return jax.shard_map(
        on_device,
        mesh=mesh,
        in_specs=(P(None, "tm", "rows", None), P(None, None, "tm", "rows", None)),
        out_specs=(P(None, "tm", "rows", None), P(None, "tm", "rows", None), P()),
        check_vma=False,
    )
```

```python
import functools

import jax
import jax.numpy as jnp
import numpy as np
from jax import lax
from jax.experimental import pallas as pl
from jax.experimental.pallas import tpu as pltpu
from jax.sharding import PartitionSpec as P

SWEEPS = 4
ALPHA = 0.01
LANES = 128
SUB = 8
GROUP = SUB // 2
FIELDS = 2
MESH = pl.DeviceIdType.MESH


def coefficients(steps):
    kappa = 16.0 / (steps * steps)
    index = np.arange(steps)
    base = ALPHA ** (1.0 / steps)
    gamma = ALPHA ** (index / steps)
    lam = 1.0 - base * np.exp(-2j * np.pi * index / steps)
    den = lam * lam + 4.0 * kappa
    wave = np.exp(2j * np.pi * (np.outer(index, index) % steps) / steps)
    scale = gamma[None, :] / gamma[:, None] / steps
    out = np.zeros((SWEEPS, FIELDS, steps, FIELDS, steps))
    for s in range(SWEEPS):
        power = kappa**s / den ** (s + 1)
        for f in range(FIELDS):
            for g in range(FIELDS):
                symbol = power * lam ** (f + 1 - g)
                if f == 1 and g == 0 and s == 0:
                    symbol = symbol - 1.0
                kernel = ((wave * symbol) @ wave.conj().T).real
                out[s, f, :, g, :] = kernel * scale
    return out.reshape(SWEEPS * FIELDS * steps, FIELDS * steps)


def split_terms(matrix):
    rest = matrix.astype(np.float32)
    pieces = []
    for _ in range(3):
        piece = rest.astype(jnp.bfloat16)
        pieces.append(piece)
        rest = rest - piece.astype(np.float32)
    one, two, three = pieces
    return np.concatenate([one, two, three, one, two, one], axis=1)


def roll(value, shift, axis):
    size = value.shape[axis]
    if isinstance(shift, int):
        shift = shift % size
        if shift == 0:
            return value
    else:
        shift = lax.rem(shift + 2 * size, size)
    return pltpu.roll(value, shift, axis)


def unpack(steps, krylov, got_out, parts, z_ref, im_ref, gram_ref):
    cols = z_ref.shape[2]
    width = cols // steps
    slot = LANES // 4
    per = LANES // width
    lane = lax.broadcasted_iota(jnp.int32, (SUB, LANES), 1)
    for tile in range(cols // LANES):
        values = [jnp.zeros((SUB, LANES), jnp.float32) for _ in range(4)]
        for i in range(per):
            source = tile * per + i
            got = got_out[source * SUB:(source + 1) * SUB, :]
            spot = (lane >= i * width) & (lane < (i + 1) * width)
            for m in range(4):
                values[m] = jnp.where(spot, roll(got, i * width - m * slot, 1), values[m])
        at = slice(tile * LANES, (tile + 1) * LANES)
        z_ref[0, :, at] = values[0]
        z_ref[1, :, at] = values[1]
        im_ref[0, :, at] = values[2]
        im_ref[1, :, at] = values[3]
    gram_ref[...] = jnp.sum(parts[...], axis=(0, 1))[: krylov + 1]


def kernel(steps, ranks, cols, krylov, x_hbm, b_hbm, c_hbm, got_out, parts,
           x_ref, b_ref, c_ref, pack_own, pack_halo, pack_basis, got_own, got_halo, got_basis,
           pack_out, part, in_sem, send_sem, recv_sem):
    me = lax.axis_index("tm")
    row = lax.axis_index("rows")
    other = 1 - row
    width = cols // steps
    span = width + 2 * SWEEPS
    slot = LANES // 4
    kappa = 16.0 / (steps * steps)
    planes = krylov * FIELDS
    tiles = planes // 4
    lane = lax.broadcasted_iota(jnp.int32, (SUB, LANES), 1)
    sub = lax.broadcasted_iota(jnp.int32, (SUB, LANES), 0)

    barrier = pltpu.get_barrier_semaphore()

    def peer(k):
        return lax.rem(me + lax.rem(k + steps // 2 - 2, steps - 1) + 1, steps)

    def greet(k, carry):
        to = peer(k)
        pl.semaphore_signal(barrier, inc=1, device_id={"tm": to, "rows": row}, device_id_type=MESH)
        pl.semaphore_signal(barrier, inc=1, device_id={"tm": to, "rows": other}, device_id_type=MESH)
        return carry

    loads = [
        pltpu.make_async_copy(x_hbm, x_ref, in_sem.at[0]),
        pltpu.make_async_copy(b_hbm, b_ref, in_sem.at[1]),
        pltpu.make_async_copy(c_hbm, c_ref, in_sem.at[2]),
    ]
    for load in loads:
        load.start()
    pl.semaphore_signal(barrier, inc=1, device_id={"tm": me, "rows": other}, device_id_type=MESH)
    lax.fori_loop(1, steps, greet, 0)

    def window(read, start, count, place):
        first = max(start, 0)
        last = min(start + count, cols)
        lo = first // LANES
        hi = (last - 1) // LANES
        shift = place - start
        at = lane - place
        value = jnp.zeros((SUB, LANES), jnp.float32)
        for tile in range(lo, hi + 1):
            left = max(first, tile * LANES) - start
            right = min(last, (tile + 1) * LANES) - start
            moved = roll(read(tile), shift + tile * LANES, 1)
            value = jnp.where((at >= left) & (at < right), moved, value)
        return value

    loads[0].wait()
    lows, highs, edges = [], [], []
    for tile in range(cols // LANES):
        at = slice(tile * LANES, (tile + 1) * LANES)
        f0, f1 = x_ref[0, :, at], x_ref[1, :, at]
        low = jnp.where(sub < GROUP, f0, roll(f1, GROUP, 0))
        high = jnp.where(sub < GROUP, roll(f0, GROUP, 0), f1)
        lows.append(low)
        highs.append(high)
        edges.append(jnp.where(row == 0, high, low))
    for to in range(steps):
        start = to * width - SWEEPS
        own = window(lambda i: lows[i], start, span, span * row)
        own = own + window(lambda i: highs[i], start, span, span * (row + 1))
        pack_own[to * SUB:(to + 1) * SUB, :] = own
        pack_halo[to * SUB:(to + 1) * SUB, :] = window(lambda i: edges[i], start, span, 2 * span * row)
    def block(index, size):
        return pl.ds(pl.multiple_of(index * size, size), size)

    def remote(source, target, size, to, to_row, which):
        return pltpu.make_async_remote_copy(
            src_ref=source.at[block(to, size)],
            dst_ref=target.at[block(me, size)],
            send_sem=send_sem.at[which],
            recv_sem=recv_sem.at[which],
            device_id={"tm": to, "rows": to_row},
            device_id_type=MESH,
        )

    def keep(source, target, size, which):
        pltpu.make_async_copy(source.at[block(me, size)], target.at[block(me, size)], recv_sem.at[which]).start()

    def arrived(target, which):
        pltpu.make_async_copy(target, target, recv_sem.at[which]).wait()

    def left(source, count, which):
        ref = source.at[pl.ds(0, count)]
        pltpu.make_async_copy(ref, ref, send_sem.at[which]).wait()

    pl.semaphore_wait(barrier, steps * ranks - 1)

    def send_resid(k, carry):
        to = peer(k)
        remote(pack_own, got_own, SUB, to, row, 0).start()
        return carry

    def send_halo(k, carry):
        remote(pack_halo, got_halo, SUB, peer(k), other, 1).start()
        return carry

    def send_basis(k, carry):
        remote(pack_basis, got_basis, SUB * tiles, peer(k), row, 2).start()
        return carry

    lax.fori_loop(1, steps, send_resid, 0)
    lax.fori_loop(1, steps, send_halo, 0)
    remote(pack_halo, got_halo, SUB, me, other, 1).start()
    keep(pack_own, got_own, SUB, 0)

    loads[1].wait()
    for to in range(steps):
        for b in range(tiles):
            value = jnp.zeros((SUB, LANES), jnp.float32)
            for m in range(4):
                plane = b * 4 + m
                read = lambda i, plane=plane: b_ref[plane // FIELDS, plane % FIELDS, :, i * LANES:(i + 1) * LANES]
                value = value + window(read, to * width, width, m * slot)
            at = (to * tiles + b) * SUB
            pack_basis[at:at + SUB, :] = value
    lax.fori_loop(1, steps, send_basis, 0)
    keep(pack_basis, got_basis, SUB * tiles, 2)
    loads[2].wait()

    arrived(got_own, 0)
    arrived(got_halo, 1)
    stripes = []
    for p in range(GROUP):
        pair = []
        for f in range(FIELDS):
            at = pl.ds(f * GROUP + p, steps, stride=SUB)
            pair.append(got_own[at, :] + got_halo[at, :])
        stripes.append(jnp.concatenate(pair, axis=0))
    data = jnp.concatenate(stripes, axis=1)
    one = data.astype(jnp.bfloat16)
    rest = data - one.astype(jnp.float32)
    two = rest.astype(jnp.bfloat16)
    three = (rest - two.astype(jnp.float32)).astype(jnp.bfloat16)
    stacked = jnp.concatenate([one, one, one, two, two, three], axis=0)
    depth = FIELDS * steps

    lane2 = lax.broadcasted_iota(jnp.int32, (depth, LANES), 1)
    column = lax.rem(lane2, span) + (me * width - SWEEPS)
    inside = (column >= 0) & (column < cols) & (lane2 < 3 * span)

    def term(s):
        product = jnp.dot(c_ref[s * depth:(s + 1) * depth, :], stacked, preferred_element_type=jnp.float32)
        return [product[:, p * LANES:(p + 1) * LANES] for p in range(GROUP)]

    def near(field):
        at = lane2[: field[0].shape[0]]
        out = []
        for p in range(GROUP):
            if p > 0:
                above = field[p - 1]
            else:
                above = jnp.where(at >= span, roll(field[GROUP - 1], span, 1), 0.0)
            if p < GROUP - 1:
                below = field[p + 1]
            else:
                below = jnp.where(at < 2 * span, roll(field[0], -span, 1), 0.0)
            out.append((above + below) + (roll(field[p], 1, 1) + roll(field[p], -1, 1)))
        return out

    field = term(SWEEPS - 1)
    for s in range(SWEEPS - 2, -1, -1):
        field = [a + jnp.where(inside, b, 0.0) for a, b in zip(term(s), near(field))]

    disp = [v[:steps] for v in field]
    vel = [v[steps:] for v in field]
    later = lax.broadcasted_iota(jnp.int32, (steps, LANES), 0) > 0
    before = lambda v: jnp.where(later, roll(v, 1, 0), 0.0)
    around = near(disp)
    lane1 = lane2[:steps]
    rows_out = [None] * SUB
    for p in range(GROUP):
        first = disp[p] - before(disp[p]) - vel[p]
        second = vel[p] - before(vel[p]) - kappa * (around[p] - 4.0 * disp[p])
        for h in range(2):
            value = jnp.zeros((steps, LANES), jnp.float32)
            for m, comp in enumerate((disp[p], vel[p], first, second)):
                moved = roll(comp, m * slot - SWEEPS - span * (row + h), 1)
                value = jnp.where((lane1 >= m * slot) & (lane1 < m * slot + width), moved, value)
            q = h * GROUP + p
            rows_out[q] = value
            pack_out[pl.ds(q, steps, stride=SUB), :] = value

    def send_out(k, carry):
        remote(pack_out, got_out, SUB, peer(k), row, 3).start()
        return carry

    lax.fori_loop(1, steps, send_out, 0)
    keep(pack_out, got_out, SUB, 3)

    arrived(got_basis, 2)
    sums = [jnp.zeros((steps, LANES), jnp.float32) for _ in range(tiles + 1)]
    for q in range(SUB):
        value = rows_out[q]
        twice = jnp.where(lane1 < 2 * slot, roll(value, 2 * slot, 1), value)
        for b in range(tiles):
            sums[b] = sums[b] + twice * got_basis[pl.ds(b * SUB + q, steps, stride=SUB * tiles), :]
        sums[tiles] = sums[tiles] + twice * twice
    lane0 = lax.broadcasted_iota(jnp.int32, (1, LANES), 1)
    line = jnp.zeros((1, LANES), jnp.float32)
    total = 2.0 * steps * ranks * SUB * cols
    for b in range(tiles + 1):
        folded = jnp.sum(sums[b], axis=0, keepdims=True)
        if b < tiles:
            low = jnp.sum(jnp.where(lane0 < 2 * slot, folded, 0.0), axis=1, keepdims=True)
            high = jnp.sum(jnp.where(lane0 >= 2 * slot, folded, 0.0), axis=1, keepdims=True)
            line = jnp.where(lane0 == 2 * b, low, jnp.where(lane0 == 2 * b + 1, high, line))
        else:
            low = jnp.sum(jnp.where(lane0 < 2 * slot, folded, 0.0), axis=1, keepdims=True)
            line = jnp.where(lane0 == krylov, low * (1.0 / total), line)
    part[...] = line[None]
    mine = me * ranks + row

    def tell(to, to_row):
        pltpu.make_async_remote_copy(
            src_ref=part,
            dst_ref=parts.at[pl.ds(mine, 1)],
            send_sem=send_sem.at[4],
            recv_sem=recv_sem.at[4],
            device_id={"tm": to, "rows": to_row},
            device_id_type=MESH,
        ).start()

    def send_part(k, carry):
        to = peer(k)
        tell(to, row)
        tell(to, other)
        return carry

    lax.fori_loop(1, steps, send_part, 0)
    tell(me, other)
    pltpu.make_async_copy(part, parts.at[pl.ds(mine, 1)], recv_sem.at[4]).start()

    arrived(got_out, 3)
    arrived(parts, 4)
    left(pack_own, (steps - 1) * SUB, 0)
    left(pack_halo, steps * SUB, 1)
    left(pack_basis, (steps - 1) * SUB * tiles, 2)
    left(pack_out, (steps - 1) * SUB, 3)
    left(parts, steps * ranks - 1, 4)


def solution(mesh):
    steps, ranks = mesh.shape["tm"], mesh.shape["rows"]
    table = split_terms(coefficients(steps))

    def on_device(resid, basis):
        rows_dev, cols = resid.shape[2:]
        krylov = basis.shape[0]
        width = cols // steps
        assert ranks == 2 and rows_dev == SUB and cols % LANES == 0 and cols % steps == 0
        assert LANES % width == 0 and 4 * width <= LANES and 3 * (width + 2 * SWEEPS) <= LANES
        assert (krylov * FIELDS) % 4 == 0 and steps % SUB == 0
        tiles = krylov * FIELDS // 4
        const = jnp.asarray(table)
        limit = 55100 * 1024
        vmem = lambda *shape: pltpu.VMEM(shape, jnp.float32)
        plane = jax.ShapeDtypeStruct((FIELDS, rows_dev, cols), jnp.float32)
        got, parts = pl.pallas_call(
            functools.partial(kernel, steps, ranks, cols, krylov),
            out_shape=[
                jax.ShapeDtypeStruct((steps * SUB, LANES), jnp.float32),
                jax.ShapeDtypeStruct((steps * ranks, 1, LANES), jnp.float32),
            ],
            in_specs=[pl.BlockSpec(memory_space=pltpu.HBM)] * 3,
            out_specs=[pl.BlockSpec(memory_space=pl.ANY)] * 2,
            scratch_shapes=[
                vmem(FIELDS, rows_dev, cols),
                vmem(krylov, FIELDS, rows_dev, cols),
                pltpu.VMEM(table.shape, jnp.bfloat16),
                vmem(steps * SUB, LANES),
                vmem(steps * SUB, LANES),
                vmem(steps * SUB * tiles, LANES),
                vmem(steps * SUB, LANES),
                vmem(steps * SUB, LANES),
                vmem(steps * SUB * tiles, LANES),
                vmem(steps * SUB, LANES),
                vmem(1, 1, LANES),
                pltpu.SemaphoreType.DMA((3,)),
                pltpu.SemaphoreType.DMA((5,)),
                pltpu.SemaphoreType.DMA((5,)),
            ],
            compiler_params=pltpu.CompilerParams(collective_id=0, has_side_effects=True, vmem_limit_bytes=limit),
        )(resid[:, 0], basis[:, :, 0], const)
        z, image, gram = pl.pallas_call(
            functools.partial(unpack, steps, krylov),
            out_shape=[plane, plane, jax.ShapeDtypeStruct((krylov + 1,), jnp.float32)],
            in_specs=[pl.BlockSpec(memory_space=pltpu.VMEM)] * 2,
            out_specs=[pl.BlockSpec(memory_space=pltpu.VMEM)] * 3,
            compiler_params=pltpu.CompilerParams(vmem_limit_bytes=32 * 1024 * 1024),
        )(got, parts)
        return z[:, None], image[:, None], gram

    return jax.shard_map(
        on_device,
        mesh=mesh,
        in_specs=(P(None, "tm", "rows", None), P(None, None, "tm", "rows", None)),
        out_specs=(P(None, "tm", "rows", None), P(None, "tm", "rows", None), P()),
        check_vma=False,
    )
```
